32 devices in a mesh: gx: 2 (over x), gy: 4 (over y, core), gz: 4 (over z).
Axes of the slice: x: 2, y: 2, z: 4, core: 2. Of those that a mesh axis runs over, the one named last changes fastest.
Arguments:
- right_side: float32 [4, 5, 2, 32, 512], P(None, None, 'gx', 'gy', 'gz'), may hold values from -6 to 6
- jacobian: bfloat16 [27, 5, 5, 2, 32, 512], P(None, None, None, 'gx', 'gy', 'gz'), may hold values from -0.14 to 12.14, as said below
Outputs:
- solution: float32 [4, 5, 2, 32, 512], P(None, None, 'gx', 'gy', 'gz')
- residual: float32 [4, 5, 2, 32, 512], P(None, None, 'gx', 'gy', 'gz')
The draws below stay inside these ranges and needn't reach their ends.
Inputs may be any that keep to these rules, and one draw needn't show every extreme that they name: `jacobian`: blocks of offsets other than 13 and the off-diagonal entries of block 13 lie within -0.14 to 0.14; the diagonal entries of block 13 exceed 5.8 in every cell.
All inputs are finite; a program needn't handle non-finite values.
Results may differ from the reference program's by a relative error of at most 0.0003.
Values sent between devices are 32-bit elements.
A program may use at most 64 MiB of HBM per device.

```python
import jax
import jax.numpy as jnp
from jax import lax

COMP = 5
RHS = 4
STENCIL = 27
ITERS = 3
NX = 2
NY = 32
NZ = 512


def draw_jacobian(key, part):
    first_key, second_key = jax.random.split(jax.random.fold_in(key, 17))
    full_shape = (STENCIL, COMP, COMP, NX, NY, NZ)
    diag_shape = (COMP, NX, NY, NZ)
    entries = jax.random.uniform(first_key, full_shape, jnp.float32, -0.14, 0.14)
    diagonal = jax.random.uniform(second_key, diag_shape, jnp.float32, 6.0, 12.0)
    identity = jnp.eye(COMP, dtype=jnp.float32)[:, :, None, None, None]
    center = entries[13] + identity * diagonal[:, None]
    entries = entries.at[13].set(center)
    return entries.astype(jnp.bfloat16)


def levels(rng, extent, shards, least, high):
    level = 1.0
    for axis_at, blocks in shards:
        heights = jax.random.uniform(jax.random.fold_in(jax.random.fold_in(rng, 6), axis_at), (blocks,), jnp.float32, least / len(shards), high / len(shards))
        level = level * jnp.repeat(jnp.exp(heights), extent[axis_at] // blocks).reshape((-1,) + (1,) * (len(extent) - 1 - axis_at))
    return level


def noise(rng, extent, deviation, bound, shards=(), kind=jnp.bfloat16):
    array = jax.random.normal(rng, extent, jnp.float32) * deviation
    if len(shards) > 0:
        array = levels(rng, extent, shards, -0.22, 0.18) * array
    return jnp.clip(array, min=-bound, max=bound).astype(kind)


def setup_inputs(seed: int = 0) -> dict:
    streams_of = jax.random.split(jax.random.key(seed), 3)
    return {
        "right_side": noise(streams_of[0], (RHS, COMP, NX, NY, NZ), 1.0, 6.0, ((2, 2), (3, 4), (4, 4)), jnp.float32),
        "jacobian": draw_jacobian(jax.random.fold_in(streams_of[2], 71), 0),
    }


def dot_high(left, right):
    return jnp.dot(left.astype(jnp.float32), right.astype(jnp.float32), precision=lax.Precision.HIGHEST, preferred_element_type=jnp.float32)

def lower_solve(factor, target):
    solved = []
    for row_pos in range(factor.shape[0]):
        accum = target[row_pos]
        for prior in range(row_pos):
            accum = accum - factor[row_pos, prior] * solved[prior]
        solved.append(accum / factor[row_pos, row_pos])
    return jnp.stack(solved)

def upper_solve(factor, target):
    size_all = factor.shape[0]
    solved = [None] * size_all
    for row_pos in range(size_all - 1, -1, -1):
        accum = target[row_pos]
        for later in range(row_pos + 1, size_all):
            accum = accum - factor[later, row_pos] * solved[later]
        solved[row_pos] = accum / factor[row_pos, row_pos]
    return jnp.stack(solved)

def extend(field):
    padded = jnp.pad(field, ((0, 0), (0, 0), (1, 1), (1, 1), (0, 0)), mode='wrap')
    return jnp.pad(padded, ((0, 0), (0, 0), (0, 0), (0, 0), (1, 1)))

def apply_operator(jacobian, padded):
    extent_x = padded.shape[2] - 2
    extent_y = padded.shape[3] - 2
    extent_z = padded.shape[4] - 2
    total = jnp.zeros((padded.shape[0], padded.shape[1], extent_x, extent_y, extent_z), jnp.float32)
    for stencil_pos in range(27):
        start_x = stencil_pos // 9
        start_y = stencil_pos // 3 % 3
        start_z = stencil_pos % 3
        piece = padded[:, :, start_x:start_x + extent_x, start_y:start_y + extent_y, start_z:start_z + extent_z]
        block = jacobian[stencil_pos].astype(jnp.float32)
        for source_comp in range(block.shape[1]):
            total = total + block[None, :, source_comp] * piece[:, source_comp][:, None]
    return total

def reference(right_side, jacobian):
    field_shape = right_side.shape
    rhs_count = field_shape[0]
    flat_rhs = right_side.reshape(rhs_count, -1)
    start_factor = jnp.linalg.cholesky(dot_high(flat_rhs, flat_rhs.T))
    basis = [lower_solve(start_factor, flat_rhs)]
    hessen_rows = []
    for iteration in range(ITERS):
        workspace = apply_operator(jacobian, extend(basis[-1].reshape(field_shape))).reshape(rhs_count, -1)
        stacked = jnp.concatenate(basis, axis=0)
        coefficients = dot_high(stacked, workspace.T)
        workspace = workspace - dot_high(coefficients.T, stacked)
        factor = jnp.linalg.cholesky(dot_high(workspace, workspace.T))
        basis.append(lower_solve(factor, workspace))
        filler = jnp.zeros((rhs_count, rhs_count * (ITERS - iteration - 1)), jnp.float32)
        hessen_rows.append(jnp.concatenate([coefficients.T, factor, filler], axis=1))
    hessen = jnp.concatenate(hessen_rows, axis=0)
    target = jnp.concatenate([start_factor, jnp.zeros((rhs_count, rhs_count * ITERS), jnp.float32)], axis=1)
    normal_factor = jnp.linalg.cholesky(dot_high(hessen, hessen.T))
    middle = lower_solve(normal_factor, dot_high(hessen, target.T))
    weights = upper_solve(normal_factor, middle)
    solution = dot_high(weights.T, jnp.concatenate(basis[:-1], axis=0))
    solution_field = solution.reshape(field_shape)
    residual = right_side - apply_operator(jacobian, extend(solution_field))
    return (solution_field, residual)
```

```python
import functools
import itertools

import jax
import jax.numpy as jnp
from jax import lax
from jax.experimental import pallas as pl
from jax.experimental.pallas import tpu as pltpu
from jax.sharding import PartitionSpec as P

ITERS = 3
SHIFT = 9.0
MESH = pl.DeviceIdType.MESH
AXES = ("gx", "gy", "gz")


def make_kernel(sizes, rhs, comp, rows, lanes):
    count_x, count_y, count_z = sizes
    devices = count_x * count_y * count_z
    fields = rhs * comp
    merged = count_x == 2
    plane_steps = (0, 1) if merged else (0, 1, -1)
    planes = len(plane_steps)
    pair_list = []
    vectors = rhs * (ITERS + 1)
    for step in range(1, ITERS + 1):
        for mine in range(rhs * step, rhs * (step + 1)):
            for other in range(0, mine + 1):
                pair_list.append((mine, other))
    pair_slot = {pair: slot for slot, pair in enumerate(pair_list)}
    pair_pad = -(-len(pair_list) // 128) * 128

    def kernel(
        right_ref, jac_hbm, sol_ref, res_ref,
        basis, prods, jac_low, jac, shifted, packs, edge_rows, edge_corner,
        far_plane, halo_rows, halo_cols, halo_corner, tops, gram, part, parts,
        jac_sem, send_sem, recv_sem, red_send, red_recv,
    ):
        my_x, my_y, my_z = (lax.axis_index(axis) for axis in AXES)
        me = (my_x * count_y + my_y) * count_z + my_z

        def coords(index):
            return (index // (count_y * count_z), index // count_z % count_y, index % count_z)

        loads = pltpu.make_async_copy(jac_hbm, jac_low, jac_sem)
        loads.start()

        barrier = pltpu.get_barrier_semaphore()

        def greet(step, carry):
            pl.semaphore_signal(
                barrier, inc=1, device_id=coords(lax.rem(me + step, devices)), device_id_type=MESH
            )
            return carry

        lax.fori_loop(1, devices, greet, 0)

        lane = lax.broadcasted_iota(jnp.int32, (rows, lanes), 1)
        sub = lax.broadcasted_iota(jnp.int32, (rows, lanes), 0)

        def field(turn, at):
            return right_ref[at] if turn == 0 else basis[turn - 1, at]

        def pack(turn):
            packed = jnp.zeros((rows, lanes), jnp.float32)
            for at in range(fields):
                value = field(turn, at)
                edge_rows[turn, 0, at : at + 1, :] = value[rows - 1 : rows]
                edge_rows[turn, 1, at : at + 1, :] = value[0:1]
                packed = jnp.where(lane // 2 == at, pltpu.roll(value, 2 * at + 1, 1), packed)
            packs[turn] = packed
            edge_corner[turn, 0] = packed[rows - 1 : rows]
            edge_corner[turn, 1] = packed[0:1]

        def messages(turn):
            found = []
            for plane, step_x in enumerate(plane_steps):
                for dy, dz in itertools.product((0, 1, -1), (0, 1, -1)):
                    side_y = 0 if dy == 1 else 1
                    side_z = 0 if dz == 1 else 1
                    if dy == 0 and dz == 0:
                        if plane == 0:
                            continue
                        source = right_ref if turn == 0 else basis.at[turn - 1]
                        target = far_plane.at[turn, plane - 1]
                    elif dz == 0:
                        source = edge_rows.at[turn, side_y]
                        target = halo_rows.at[turn, plane, side_y]
                    elif dy == 0:
                        source = packs.at[turn]
                        target = halo_cols.at[turn, plane, side_z]
                    else:
                        source = edge_corner.at[turn, side_y]
                        target = halo_corner.at[turn, plane, side_y, side_z]
                    slot = plane * 9 + (dy + 1) * 3 + dz + 1
                    copy = pltpu.make_async_remote_copy(
                        src_ref=source,
                        dst_ref=target,
                        send_sem=send_sem.at[turn, slot],
                        recv_sem=recv_sem.at[turn, slot],
                        device_id=(
                            lax.rem(my_x + step_x + count_x, count_x),
                            lax.rem(my_y + dy + count_y, count_y),
                            jnp.clip(my_z + dz, 0, count_z - 1),
                        ),
                        device_id_type=MESH,
                    )
                    found.append((plane, dz, copy))
            return found

        above = my_z < count_z - 1
        below = my_z > 0

        def for_each(copies, act, sending):
            for step_z in (1, -1, 0):
                chosen = [copy for _, dz, copy in copies if dz == step_z]
                if step_z == 0:
                    for copy in chosen:
                        act(copy)
                else:
                    present = above if (step_z == 1) == sending else below

                    @pl.when(present)
                    def _():
                        for copy in chosen:
                            act(copy)

        def shift_plane(turn, plane):
            low = jnp.where(below, pltpu.roll(halo_cols[turn, plane, 0], 1, 1), 0.0)
            high = jnp.where(above, pltpu.roll(halo_cols[turn, plane, 1], lanes - 1, 1), 0.0)
            mixed = jnp.where(lane % 2 == 1, low, high)
            wide_lane = lax.broadcasted_iota(jnp.int32, (fields, lanes), 1)
            wide_at = lax.broadcasted_iota(jnp.int32, (fields, lanes), 0)
            for side in range(2):
                strip = halo_rows[turn, plane, side]
                low_row = jnp.where(below, halo_corner[turn, plane, side, 0], 0.0)
                high_row = jnp.where(above, halo_corner[turn, plane, side, 1], 0.0)
                low_col = jnp.sum(
                    jnp.where(wide_lane == 2 * wide_at, low_row, 0.0), axis=1, keepdims=True
                )
                high_col = jnp.sum(
                    jnp.where(wide_lane == 2 * wide_at + 1, high_row, 0.0), axis=1, keepdims=True
                )
                tops[side, 0] = jnp.where(wide_lane == 0, low_col, pltpu.roll(strip, 1, 1))
                tops[side, 1] = strip
                tops[side, 2] = jnp.where(
                    wide_lane == lanes - 1, high_col, pltpu.roll(strip, lanes - 1, 1)
                )
            for at in range(fields):
                value = field(turn, at) if plane == 0 else far_plane[turn, plane - 1, at]
                edge = pltpu.roll(mixed, lanes - 2 * at - 1, 1)
                along = (
                    jnp.where(lane == 0, edge, pltpu.roll(value, 1, 1)),
                    value,
                    jnp.where(lane == lanes - 1, edge, pltpu.roll(value, lanes - 1, 1)),
                )
                for dz in range(3):
                    shifted[dz, at] = jnp.where(
                        sub == 0, tops[0, dz, at : at + 1, :], pltpu.roll(along[dz], 1, 0)
                    )
                    shifted[3 + dz, at] = along[dz]
                    shifted[6 + dz, at] = jnp.where(
                        sub == rows - 1,
                        tops[1, dz, at : at + 1, :],
                        pltpu.roll(along[dz], rows - 1, 0),
                    )

        def stencil(plane, totals):
            def body(near, sums):
                sums = list(sums)
                for source in range(comp):
                    blocks = [jac[plane, near, a * comp + source] for a in range(comp)]
                    for r in range(rhs):
                        value = shifted[near, r * comp + source]
                        for a in range(comp):
                            sums[r * comp + a] = sums[r * comp + a] + blocks[a] * value
                return tuple(sums)

            return lax.fori_loop(0, 9, body, totals)

        def vector(index, c):
            if index < rhs:
                return right_ref[index * comp + c]
            return prods[index // rhs - 1, (index % rhs) * comp + c]

        def dots(step):
            for mine in range(rhs * step, rhs * (step + 1)):
                own = [vector(mine, c) for c in range(comp)]
                for other in range(0, mine + 1):
                    total = own[0] * vector(other, 0)
                    for c in range(1, comp):
                        total = total + own[c] * vector(other, c)
                    gram[pair_slot[mine, other]] = total

        for slot in range(len(pair_list), pair_pad):
            gram[slot] = jnp.zeros((rows, lanes), jnp.float32)
        pack(0)
        pl.semaphore_wait(barrier, devices - 1)

        for turn in range(ITERS):
            copies = messages(turn)
            for_each(copies, lambda copy: copy.start(), True)
            if turn == 0:
                loads.wait()

                def widen(near, carry):
                    for entry in range(comp * comp):
                        jac[0, near, entry] = jac_low[9 + near, entry].astype(jnp.float32)
                        first = jac_low[near, entry].astype(jnp.float32)
                        last = jac_low[18 + near, entry].astype(jnp.float32)
                        if merged:
                            jac[1, near, entry] = first + last
                        else:
                            jac[1, near, entry] = first
                            jac[2, near, entry] = last
                    return carry

                lax.fori_loop(0, 9, widen, 0)
            else:
                dots(turn)
            totals = tuple(jnp.zeros((rows, lanes), jnp.float32) for _ in range(fields))
            for plane in range(planes):
                mine = [copy for copy in copies if copy[0] == plane]
                for_each(mine, lambda copy: copy.wait_recv(), False)
                shift_plane(turn, plane)
                totals = stencil(plane, totals)
            for at in range(fields):
                prods[turn, at] = totals[at]
                if turn < ITERS - 1:
                    basis[turn, at] = totals[at] - SHIFT * field(turn, at)
            if turn < ITERS - 1:
                pack(turn + 1)

        dots(ITERS)
        sums = jnp.sum(gram[...], axis=1)
        row = lax.dot_general(
            jnp.ones((rows, lanes), jnp.float32),
            sums,
            (((1,), (1,)), ((), ())),
            precision=lax.Precision.HIGHEST,
            preferred_element_type=jnp.float32,
        )
        part[...] = row[0:1]

        def spread(step):
            return pltpu.make_async_remote_copy(
                src_ref=part,
                dst_ref=parts.at[me],
                send_sem=red_send.at[step],
                recv_sem=red_recv.at[step],
                device_id=coords(lax.rem(me + step, devices)),
                device_id_type=MESH,
            )

        def gathered(step):
            return pltpu.make_async_remote_copy(
                src_ref=part,
                dst_ref=parts.at[lax.rem(me + devices - step, devices)],
                send_sem=red_send.at[step],
                recv_sem=red_recv.at[step],
                device_id=coords(lax.rem(me + step, devices)),
                device_id_type=MESH,
            )

        def begin(step, carry):
            spread(step).start()
            return carry

        def finish(step, carry):
            gathered(step).wait_recv()
            return carry

        lax.fori_loop(1, devices, begin, 0)
        parts[me] = part[...]
        lax.fori_loop(1, devices, finish, 0)
        total_row = jnp.broadcast_to(jnp.sum(parts[...], axis=0), (rows, pair_pad))

        def entry(mine, other):
            slot = pair_slot[max(mine, other), min(mine, other)]
            return jnp.broadcast_to(total_row[:, slot : slot + 1], (rows, lanes))

        size = rhs * ITERS
        matrix = {}
        target = {}
        for i in range(size):
            for j in range(i + 1):
                matrix[i, j] = entry(rhs + i, rhs + j)
            for r in range(rhs):
                target[i, r] = entry(rhs + i, r)
        inverse = {}
        for k in range(size):
            inverse[k] = 1.0 / matrix[k, k]
            for i in range(k + 1, size):
                ratio = matrix[i, k] * inverse[k]
                for j in range(k + 1, i + 1):
                    matrix[i, j] = matrix[i, j] - ratio * matrix[j, k]
                for r in range(rhs):
                    target[i, r] = target[i, r] - ratio * target[k, r]
        weights = {}
        for k in range(size - 1, -1, -1):
            for r in range(rhs):
                accum = target[k, r]
                for later in range(k + 1, size):
                    accum = accum - matrix[later, k] * weights[later, r]
                weights[k, r] = accum * inverse[k]
        for r in range(rhs):
            for c in range(comp):
                found = jnp.zeros((rows, lanes), jnp.float32)
                left = right_ref[r * comp + c]
                for j in range(size):
                    found = found + weights[j, r] * field(j // rhs, (j % rhs) * comp + c)
                    left = left - weights[j, r] * prods[j // rhs, (j % rhs) * comp + c]
                sol_ref[r * comp + c] = found
                res_ref[r * comp + c] = left

        for turn in range(ITERS):
            for_each(messages(turn), lambda copy: copy.wait_send(), True)

        def settle(step, carry):
            spread(step).wait_send()
            return carry

        lax.fori_loop(1, devices, settle, 0)

    full = (rows, lanes)
    scratch = [
        pltpu.VMEM((ITERS - 1, fields) + full, jnp.float32),
        pltpu.VMEM((ITERS, fields) + full, jnp.float32),
        pltpu.VMEM((27, comp * comp) + full, jnp.bfloat16),
        pltpu.VMEM((planes, 9, comp * comp) + full, jnp.float32),
        pltpu.VMEM((9, fields) + full, jnp.float32),
        pltpu.VMEM((ITERS,) + full, jnp.float32),
        pltpu.VMEM((ITERS, 2, fields, lanes), jnp.float32),
        pltpu.VMEM((ITERS, 2, 1, lanes), jnp.float32),
        pltpu.VMEM((ITERS, planes - 1, fields) + full, jnp.float32),
        pltpu.VMEM((ITERS, planes, 2, fields, lanes), jnp.float32),
        pltpu.VMEM((ITERS, planes, 2) + full, jnp.float32),
        pltpu.VMEM((ITERS, planes, 2, 2, 1, lanes), jnp.float32),
        pltpu.VMEM((2, 3, fields, lanes), jnp.float32),
        pltpu.VMEM((pair_pad,) + full, jnp.float32),
        pltpu.VMEM((1, pair_pad), jnp.float32),
        pltpu.VMEM((devices, 1, pair_pad), jnp.float32),
        pltpu.SemaphoreType.DMA,
        pltpu.SemaphoreType.DMA((ITERS, planes * 9)),
        pltpu.SemaphoreType.DMA((ITERS, planes * 9)),
        pltpu.SemaphoreType.DMA((devices,)),
        pltpu.SemaphoreType.DMA((devices,)),
    ]
    return kernel, scratch


def shards(sizes, right_side, jacobian):
    rhs, comp, extent_x, rows, lanes = right_side.shape
    assert extent_x == 1
    kernel, scratch = make_kernel(sizes, rhs, comp, rows, lanes)
    shape = jax.ShapeDtypeStruct((rhs * comp, rows, lanes), jnp.float32)
    vmem = pl.BlockSpec(memory_space=pltpu.VMEM)
    found, left = pl.pallas_call(
        kernel,
        out_shape=(shape, shape),
        in_specs=[vmem, pl.BlockSpec(memory_space=pl.ANY)],
        out_specs=(vmem, vmem),
        scratch_shapes=scratch,
        compiler_params=pltpu.CompilerParams(collective_id=0, has_side_effects=True),
    )(
        right_side.reshape(rhs * comp, rows, lanes),
        jacobian.reshape(27, comp * comp, rows, lanes),
    )
    return found.reshape(right_side.shape), left.reshape(right_side.shape)


def solution(mesh):
    sizes = tuple(mesh.shape[axis] for axis in AXES)
    in_specs = (P(None, None, *AXES), P(None, None, None, *AXES))
    out_specs = (P(None, None, *AXES), P(None, None, *AXES))
    return jax.shard_map(
        functools.partial(shards, sizes), mesh=mesh, in_specs=in_specs, out_specs=out_specs, check_vma=False
    )
```

```python
import functools
import itertools

import jax
import jax.numpy as jnp
from jax import lax
from jax.experimental import pallas as pl
from jax.experimental.pallas import tpu as pltpu
from jax.sharding import PartitionSpec as P

ITERS = 3
SHIFT = 9.0
MESH = pl.DeviceIdType.MESH
AXES = ("gx", "gy", "gz")


def make_kernel(sizes, rhs, comp, rows, lanes):
    count_x, count_y, count_z = sizes
    devices = count_x * count_y * count_z
    fields = rhs * comp
    merged = count_x == 2
    plane_steps = (0, 1) if merged else (0, 1, -1)
    planes = len(plane_steps)
    slots = 9 + rhs
    pair_list = []
    vectors = rhs * (ITERS + 1)
    for step in range(1, ITERS + 1):
        for mine in range(rhs * step, rhs * (step + 1)):
            for other in range(0, mine + 1):
                pair_list.append((mine, other))
    pair_slot = {pair: slot for slot, pair in enumerate(pair_list)}
    pair_pad = -(-len(pair_list) // 128) * 128

    def kernel(
        right_ref, jac_hbm, sol_ref, res_ref,
        basis, prods, jac_low, jac, shifted, packs, edge_rows, edge_corner,
        far_plane, halo_rows, halo_cols, halo_corner, tops, gram, part, parts,
        jac_sem, send_sem, recv_sem, red_send, red_recv,
    ):
        my_x, my_y, my_z = (lax.axis_index(axis) for axis in AXES)
        me = (my_x * count_y + my_y) * count_z + my_z

        def coords(index):
            return (index // (count_y * count_z), index // count_z % count_y, index % count_z)

        loads = pltpu.make_async_copy(jac_hbm, jac_low, jac_sem)
        loads.start()

        barrier = pltpu.get_barrier_semaphore()

        def greet(step, carry):
            pl.semaphore_signal(
                barrier, inc=1, device_id=coords(lax.rem(me + step, devices)), device_id_type=MESH
            )
            return carry

        lax.fori_loop(1, devices, greet, 0)

        lane = lax.broadcasted_iota(jnp.int32, (rows, lanes), 1)
        sub = lax.broadcasted_iota(jnp.int32, (rows, lanes), 0)

        def field(turn, at):
            return right_ref[at] if turn == 0 else basis[turn - 1, at]

        def pack(turn):
            packed = jnp.zeros((rows, lanes), jnp.float32)
            for at in range(fields):
                value = field(turn, at)
                edge_rows[turn, 0, at : at + 1, :] = value[rows - 1 : rows]
                edge_rows[turn, 1, at : at + 1, :] = value[0:1]
                packed = jnp.where(lane // 2 == at, pltpu.roll(value, 2 * at + 1, 1), packed)
            packs[turn] = packed
            edge_corner[turn, 0] = packed[rows - 1 : rows]
            edge_corner[turn, 1] = packed[0:1]

        def messages(turn):
            found = []
            for plane, step_x in enumerate(plane_steps):
                for dy, dz in itertools.product((1, -1, 0), (1, -1, 0)):
                    side_y = 0 if dy == 1 else 1
                    side_z = 0 if dz == 1 else 1
                    if dy == 0 and dz == 0:
                        if plane == 0:
                            continue
                        values = right_ref if turn == 0 else basis.at[turn - 1]
                        moves = [
                            (values.at[pl.ds(r * comp, comp)], far_plane.at[turn, plane - 1, pl.ds(r * comp, comp)])
                            for r in range(rhs)
                        ]
                    elif dz == 0:
                        moves = [(edge_rows.at[turn, side_y], halo_rows.at[turn, plane, side_y])]
                    elif dy == 0:
                        moves = [(packs.at[turn], halo_cols.at[turn, plane, side_z])]
                    else:
                        moves = [(edge_corner.at[turn, side_y], halo_corner.at[turn, plane, side_y, side_z])]
                    for part_at, (source, target) in enumerate(moves):
                        slot = plane * slots
                        if len(moves) == 1:
                            slot = slot + (dy + 1) * 3 + dz + 1
                        else:
                            slot = slot + 9 + part_at
                        copy = pltpu.make_async_remote_copy(
                            src_ref=source,
                            dst_ref=target,
                            send_sem=send_sem.at[turn, slot],
                            recv_sem=recv_sem.at[turn, slot],
                            device_id=(
                                lax.rem(my_x + step_x + count_x, count_x),
                                lax.rem(my_y + dy + count_y, count_y),
                                jnp.clip(my_z + dz, 0, count_z - 1),
                            ),
                            device_id_type=MESH,
                        )
                        found.append((plane, dz, copy, part_at if len(moves) > 1 else None))
            return found

        above = my_z < count_z - 1
        below = my_z > 0

        def for_each(copies, act, sending):
            for step_z in (1, -1, 0):
                chosen = [copy for _, dz, copy, _ in copies if dz == step_z]
                if step_z == 0:
                    for copy in chosen:
                        act(copy)
                else:
                    present = above if (step_z == 1) == sending else below

                    @pl.when(present)
                    def _():
                        for copy in chosen:
                            act(copy)

        def shift_edges(turn, plane):
            low = jnp.where(below, pltpu.roll(halo_cols[turn, plane, 0], 1, 1), 0.0)
            high = jnp.where(above, pltpu.roll(halo_cols[turn, plane, 1], lanes - 1, 1), 0.0)
            mixed = jnp.where(lane % 2 == 1, low, high)
            wide_lane = lax.broadcasted_iota(jnp.int32, (fields, lanes), 1)
            wide_at = lax.broadcasted_iota(jnp.int32, (fields, lanes), 0)
            for side in range(2):
                strip = halo_rows[turn, plane, side]
                low_row = jnp.where(below, halo_corner[turn, plane, side, 0], 0.0)
                high_row = jnp.where(above, halo_corner[turn, plane, side, 1], 0.0)
                low_col = jnp.sum(
                    jnp.where(wide_lane == 2 * wide_at, low_row, 0.0), axis=1, keepdims=True
                )
                high_col = jnp.sum(
                    jnp.where(wide_lane == 2 * wide_at + 1, high_row, 0.0), axis=1, keepdims=True
                )
                tops[side, 0] = jnp.where(wide_lane == 0, low_col, pltpu.roll(strip, 1, 1))
                tops[side, 1] = strip
                tops[side, 2] = jnp.where(
                    wide_lane == lanes - 1, high_col, pltpu.roll(strip, lanes - 1, 1)
                )
            return mixed

        def shift_fields(turn, plane, mixed, first, last):
            for at in range(first, last):
                value = field(turn, at) if plane == 0 else far_plane[turn, plane - 1, at]
                edge = pltpu.roll(mixed, lanes - 2 * at - 1, 1)
                along = (
                    jnp.where(lane == 0, edge, pltpu.roll(value, 1, 1)),
                    value,
                    jnp.where(lane == lanes - 1, edge, pltpu.roll(value, lanes - 1, 1)),
                )
                for dz in range(3):
                    shifted[dz, at] = jnp.where(
                        sub == 0, tops[0, dz, at : at + 1, :], pltpu.roll(along[dz], 1, 0)
                    )
                    shifted[3 + dz, at] = along[dz]
                    shifted[6 + dz, at] = jnp.where(
                        sub == rows - 1,
                        tops[1, dz, at : at + 1, :],
                        pltpu.roll(along[dz], rows - 1, 0),
                    )

        def stencil(plane, totals, sides):
            def body(line, sums):
                sums = list(sums)
                for near, source in itertools.product(range(3), range(comp)):
                    near = line * 3 + near
                    blocks = [jac[plane, near, a * comp + source] for a in range(comp)]
                    for place, r in enumerate(sides):
                        value = shifted[near, r * comp + source]
                        for a in range(comp):
                            sums[place * comp + a] = sums[place * comp + a] + blocks[a] * value
                return tuple(sums)

            return list(lax.fori_loop(0, 3, body, tuple(totals)))

        def vector(index, c):
            if index < rhs:
                return right_ref[index * comp + c]
            return prods[index // rhs - 1, (index % rhs) * comp + c]

        def dots(step):
            for mine in range(rhs * step, rhs * (step + 1)):
                own = [vector(mine, c) for c in range(comp)]
                for other in range(0, mine + 1):
                    total = own[0] * vector(other, 0)
                    for c in range(1, comp):
                        total = total + own[c] * vector(other, c)
                    gram[pair_slot[mine, other]] = total

        for slot in range(len(pair_list), pair_pad):
            gram[slot] = jnp.zeros((rows, lanes), jnp.float32)
        pack(0)
        loads.wait()

        def widen(near, carry):
            for entry in range(comp * comp):
                jac[0, near, entry] = jac_low[9 + near, entry].astype(jnp.float32)
                first = jac_low[near, entry].astype(jnp.float32)
                last = jac_low[18 + near, entry].astype(jnp.float32)
                if merged:
                    jac[1, near, entry] = first + last
                else:
                    jac[1, near, entry] = first
                    jac[2, near, entry] = last
            return carry

        lax.fori_loop(0, 9, widen, 0)
        pl.semaphore_wait(barrier, devices - 1)

        for turn in range(ITERS):
            copies = messages(turn)
            for_each(copies, lambda copy: copy.start(), True)
            if turn > 0:
                dots(turn)
            totals = [jnp.zeros((rows, lanes), jnp.float32) for _ in range(fields)]
            for plane in range(planes):
                mine = [copy for copy in copies if copy[0] == plane and copy[3] is None]
                for_each(mine, lambda copy: copy.wait_recv(), False)
                mixed = shift_edges(turn, plane)
                if plane == 0:
                    shift_fields(turn, plane, mixed, 0, fields)
                    totals = stencil(plane, totals, range(rhs))
                    for at in range(fields):
                        prods[turn, at] = totals[at]
                    continue
                for r in range(rhs):
                    for copy in copies:
                        if copy[0] == plane and copy[3] == r:
                            copy[2].wait_recv()
                    span = range(r * comp, (r + 1) * comp)
                    shift_fields(turn, plane, mixed, span.start, span.stop)
                    sums = stencil(plane, [prods[turn, at] for at in span], (r,))
                    for at, value in zip(span, sums):
                        prods[turn, at] = value
                        if turn < ITERS - 1 and plane == planes - 1:
                            basis[turn, at] = value - SHIFT * field(turn, at)
            if turn < ITERS - 1:
                pack(turn + 1)

        dots(ITERS)
        sums = jnp.sum(gram[...], axis=1)
        row = lax.dot_general(
            jnp.ones((rows, lanes), jnp.float32),
            sums,
            (((1,), (1,)), ((), ())),
            precision=lax.Precision.HIGHEST,
            preferred_element_type=jnp.float32,
        )
        part[...] = row[0:1]

        def spread(step):
            return pltpu.make_async_remote_copy(
                src_ref=part,
                dst_ref=parts.at[me],
                send_sem=red_send.at[step],
                recv_sem=red_recv.at[step],
                device_id=coords(lax.rem(me + step, devices)),
                device_id_type=MESH,
            )

        def gathered(step):
            return pltpu.make_async_remote_copy(
                src_ref=part,
                dst_ref=parts.at[lax.rem(me + devices - step, devices)],
                send_sem=red_send.at[step],
                recv_sem=red_recv.at[step],
                device_id=coords(lax.rem(me + step, devices)),
                device_id_type=MESH,
            )

        def begin(step, carry):
            spread(step).start()
            return carry

        def finish(step, carry):
            gathered(step).wait_recv()
            return carry

        lax.fori_loop(1, devices, begin, 0)
        parts[me] = part[...]
        lax.fori_loop(1, devices, finish, 0)
        total_row = jnp.broadcast_to(jnp.sum(parts[...], axis=0), (rows, pair_pad))

        def entry(mine, other):
            slot = pair_slot[max(mine, other), min(mine, other)]
            return jnp.broadcast_to(total_row[:, slot : slot + 1], (rows, lanes))

        size = rhs * ITERS
        matrix = {}
        target = {}
        for i in range(size):
            for j in range(i + 1):
                matrix[i, j] = entry(rhs + i, rhs + j)
            for r in range(rhs):
                target[i, r] = entry(rhs + i, r)
        inverse = {}
        for k in range(size):
            inverse[k] = 1.0 / matrix[k, k]
            for i in range(k + 1, size):
                ratio = matrix[i, k] * inverse[k]
                for j in range(k + 1, i + 1):
                    matrix[i, j] = matrix[i, j] - ratio * matrix[j, k]
                for r in range(rhs):
                    target[i, r] = target[i, r] - ratio * target[k, r]
        weights = {}
        for k in range(size - 1, -1, -1):
            for r in range(rhs):
                accum = target[k, r]
                for later in range(k + 1, size):
                    accum = accum - matrix[later, k] * weights[later, r]
                weights[k, r] = accum * inverse[k]
        for r in range(rhs):
            for c in range(comp):
                found = jnp.zeros((rows, lanes), jnp.float32)
                left = right_ref[r * comp + c]
                for j in range(size):
                    found = found + weights[j, r] * field(j // rhs, (j % rhs) * comp + c)
                    left = left - weights[j, r] * prods[j // rhs, (j % rhs) * comp + c]
                sol_ref[r * comp + c] = found
                res_ref[r * comp + c] = left

        for turn in range(ITERS):
            for_each(messages(turn), lambda copy: copy.wait_send(), True)

        def settle(step, carry):
            spread(step).wait_send()
            return carry

        lax.fori_loop(1, devices, settle, 0)

    full = (rows, lanes)
    scratch = [
        pltpu.VMEM((ITERS - 1, fields) + full, jnp.float32),
        pltpu.VMEM((ITERS, fields) + full, jnp.float32),
        pltpu.VMEM((27, comp * comp) + full, jnp.bfloat16),
        pltpu.VMEM((planes, 9, comp * comp) + full, jnp.float32),
        pltpu.VMEM((9, fields) + full, jnp.float32),
        pltpu.VMEM((ITERS,) + full, jnp.float32),
        pltpu.VMEM((ITERS, 2, fields, lanes), jnp.float32),
        pltpu.VMEM((ITERS, 2, 1, lanes), jnp.float32),
        pltpu.VMEM((ITERS, planes - 1, fields) + full, jnp.float32),
        pltpu.VMEM((ITERS, planes, 2, fields, lanes), jnp.float32),
        pltpu.VMEM((ITERS, planes, 2) + full, jnp.float32),
        pltpu.VMEM((ITERS, planes, 2, 2, 1, lanes), jnp.float32),
        pltpu.VMEM((2, 3, fields, lanes), jnp.float32),
        pltpu.VMEM((pair_pad,) + full, jnp.float32),
        pltpu.VMEM((1, pair_pad), jnp.float32),
        pltpu.VMEM((devices, 1, pair_pad), jnp.float32),
        pltpu.SemaphoreType.DMA,
        pltpu.SemaphoreType.DMA((ITERS, planes * slots)),
        pltpu.SemaphoreType.DMA((ITERS, planes * slots)),
        pltpu.SemaphoreType.DMA((devices,)),
        pltpu.SemaphoreType.DMA((devices,)),
    ]
    return kernel, scratch


def hand_over(found_ref, left_ref, sol_ref, res_ref):
    sol_ref[...] = found_ref[...]
    res_ref[...] = left_ref[...]


def shards(sizes, right_side, jacobian):
    rhs, comp, extent_x, rows, lanes = right_side.shape
    assert extent_x == 1
    kernel, scratch = make_kernel(sizes, rhs, comp, rows, lanes)
    shape = jax.ShapeDtypeStruct((rhs * comp, rows, lanes), jnp.float32)
    vmem = pl.BlockSpec(memory_space=pltpu.VMEM)
    found, left = pl.pallas_call(
        kernel,
        out_shape=(shape, shape),
        in_specs=[vmem, pl.BlockSpec(memory_space=pl.ANY)],
        out_specs=(vmem, vmem),
        scratch_shapes=scratch,
        compiler_params=pltpu.CompilerParams(collective_id=0, has_side_effects=True),
    )(
        right_side.reshape(rhs * comp, rows, lanes),
        jacobian.reshape(27, comp * comp, rows, lanes),
    )
    found, left = pl.pallas_call(
        hand_over,
        out_shape=(shape, shape),
        in_specs=[vmem, vmem],
        out_specs=(vmem, vmem),
    )(found, left)
    return found.reshape(right_side.shape), left.reshape(right_side.shape)


def solution(mesh):
    sizes = tuple(mesh.shape[axis] for axis in AXES)
    in_specs = (P(None, None, *AXES), P(None, None, None, *AXES))
    out_specs = (P(None, None, *AXES), P(None, None, *AXES))
    return jax.shard_map(
        functools.partial(shards, sizes), mesh=mesh, in_specs=in_specs, out_specs=out_specs, check_vma=False
    )
```
